32 devices in a mesh: island: 4 (over z), shard: 8 (over y, x, core).
Axes of the slice: x: 2, y: 2, z: 4, core: 2. Of those that a mesh axis runs over, the one named last changes fastest.
Arguments:
- weight_master: float32 [4096, 4096], P('island', 'shard'), may hold values from -6 to 6
- gain_master: float32 [4096], P(('shard', 'island')), may hold values from 0.5 to 1.5
- weight_moment: float32 [4096, 4096], P('island', 'shard'), may hold values from -0.3 to 0.3
- gain_moment: float32 [4096], P(('shard', 'island')), may hold values from -0.3 to 0.3
- attended: bfloat16 [4, 2, 768, 4096], P('island', None, 'shard'), may hold values from -6 to 6
- stream: bfloat16 [4, 2, 768, 4096], P('island', None, None, 'shard'), may hold values from -6 to 6
- targets: bfloat16 [4, 2, 768, 4096], P('island', None, None, 'shard'), may hold values from -6 to 6
Outputs:
- weight_updated: float32 [4096, 4096], P('island', 'shard')
- gain_updated: float32 [4096], P(('shard', 'island'))
- weight_velocity: float32 [4096, 4096], P('island', 'shard')
- gain_velocity: float32 [4096], P(('shard', 'island'))
The draws below stay inside these ranges and needn't reach their ends.
All inputs are finite; a program needn't handle non-finite values.
Results may differ from the reference program's by a relative error of at most 0.0066.
Values may be sent and summed in bfloat16 or wider, within the bound.
A program may use at most 192 MiB of HBM per device.

```python
import jax
import jax.numpy as jnp
from jax import lax

D = 4096
STEPS = 2
TOK = 768
ISLANDS = 4
N_ISLAND = 4


def block_scale(own_key, shape, split, smallest, largest):
    loudness, own = 1.0, jax.random.fold_in(own_key, 6)
    for position, parts in split:
        heights = jnp.exp(jax.random.uniform(jax.random.fold_in(own, position), (parts,), jnp.float32, smallest / len(split), largest / len(split)))
        loudness = loudness * jnp.repeat(heights, shape[position] // parts).reshape([-1 if axis == position else 1 for axis in range(len(shape))])
    return loudness


def normal_values(own_key, extent, width, reach, shards=(), kind=jnp.bfloat16):
    result = width * jax.random.normal(own_key, extent, jnp.float32)
    if shards:
        result = result * block_scale(own_key, extent, shards, -0.22, 0.18)
    return jnp.clip(result, -reach, reach).astype(kind)


def setup_inputs(seed: int = 0) -> dict:
    arg_keys = jax.random.split(jax.random.key(seed), 8)
    return {
        "weight_master": normal_values(arg_keys[0], (D, D), 1.0, 6.0, ((0, 4), (1, 8)), jnp.float32),
        "gain_master": jnp.clip(1.0 + 0.1 * jax.random.normal(arg_keys[1], (D,), jnp.float32), 0.5, 1.5),
        "weight_moment": normal_values(arg_keys[2], (D, D), 0.05, 0.3, ((0, 4), (1, 8)), jnp.float32),
        "gain_moment": normal_values(arg_keys[3], (D,), 0.05, 0.3, ((0, 32),), jnp.float32),
        "attended": normal_values(arg_keys[4], (ISLANDS, STEPS, TOK, D), 1.0, 6.0, ((0, 4), (2, 8))),
        "stream": normal_values(arg_keys[5], (ISLANDS, STEPS, TOK, D), 1.0, 6.0, ((0, 4), (3, 8))),
        "targets": normal_values(arg_keys[6], (ISLANDS, STEPS, TOK, D), 1.0, 6.0, ((0, 4), (3, 8))),
    }


norm_epsilon = 1e-05
inner_rate = 0.05
beta_one = 0.9
beta_two = 0.95
adam_epsilon = 0.3
decay_rate = 0.1
outer_rate = 0.7
outer_momentum = 0.9

def optimizer_update(param, gradient, first, second, number, decay):
    first = beta_one * first + (1.0 - beta_one) * gradient
    second = beta_two * second + (1.0 - beta_two) * gradient * gradient
    first_hat = first / (1.0 - beta_one ** number)
    second_hat = second / (1.0 - beta_two ** number)
    param = param - inner_rate * (first_hat / (jnp.sqrt(second_hat) + adam_epsilon) + decay * param)
    return (param, first, second)

def rounded(value):
    return lax.optimization_barrier(value.astype(jnp.bfloat16)).astype(jnp.float32)

def island_window(weight_anchor, gain_anchor, attended_all, stream_all, goals_all):
    highest = lax.Precision.HIGHEST
    width_scale = D ** (-0.5)
    weight = weight_anchor
    gain = gain_anchor
    weight_first = jnp.zeros_like(weight)
    weight_second = jnp.zeros_like(weight)
    gain_first = jnp.zeros_like(gain)
    gain_second = jnp.zeros_like(gain)
    for inner_step in range(STEPS):
        number = inner_step + 1
        weight_low = weight.astype(jnp.bfloat16).astype(jnp.float32)
        rows_wide = attended_all[inner_step].astype(jnp.float32)
        projected = jnp.dot(rows_wide, weight_low, precision=highest) * width_scale
        residual = stream_all[inner_step].astype(jnp.float32) + projected
        inverse = lax.rsqrt(lax.optimization_barrier(jnp.mean(residual * residual, axis=1, keepdims=True)) + norm_epsilon)
        normed = residual * inverse * gain
        loss_grad = rounded(normed - goals_all[inner_step].astype(jnp.float32))
        scaled = loss_grad * gain
        slope = lax.optimization_barrier(jnp.sum(scaled * residual, axis=1, keepdims=True))
        residual_grad = rounded(inverse * scaled - residual * inverse * inverse * inverse * slope / D)
        weight_grad = jnp.dot(rows_wide.T, residual_grad, precision=highest) * width_scale
        gain_grad = lax.optimization_barrier(jnp.sum(loss_grad * residual * inverse, axis=0))
        weight, weight_first, weight_second = optimizer_update(weight, weight_grad, weight_first, weight_second, number, decay_rate)
        gain, gain_first, gain_second = optimizer_update(gain, gain_grad, gain_first, gain_second, number, 0.0)
    return (weight, gain)

def reference(weight_master, gain_master, weight_moment, gain_moment, attended, stream, targets):
    weight_anchor = rounded(weight_master)
    gain_anchor = rounded(gain_master)
    weight_total = jnp.zeros_like(weight_master)
    gain_total = jnp.zeros_like(gain_master)
    for island in range(N_ISLAND):
        weight_final, gain_final = island_window(weight_anchor, gain_anchor, attended[island], stream[island], targets[island])
        weight_total = weight_total + (weight_anchor - weight_final)
        gain_total = gain_total + (gain_anchor - gain_final)
    weight_pseudo = weight_total / N_ISLAND
    gain_pseudo = gain_total / N_ISLAND
    weight_velocity = outer_momentum * weight_moment + weight_pseudo
    gain_velocity = outer_momentum * gain_moment + gain_pseudo
    weight_updated = weight_master - outer_rate * (weight_pseudo + outer_momentum * weight_velocity)
    gain_updated = gain_master - outer_rate * (gain_pseudo + outer_momentum * gain_velocity)
    return (weight_updated, gain_updated, weight_velocity, gain_velocity)
```

```python
import functools

import jax
import jax.numpy as jnp
from jax import lax
from jax.experimental import pallas as pl
from jax.experimental.pallas import tpu as pltpu
from jax.sharding import PartitionSpec as P

norm_epsilon = 1e-05
inner_rate = 0.05
beta_one = 0.9
beta_two = 0.95
adam_epsilon = 0.3
decay_rate = 0.1
outer_rate = 0.7
outer_momentum = 0.9

MESH = pl.DeviceIdType.MESH
LANES = 128
keep = 1.0 - inner_rate * decay_rate


def flip(index, bit):
    size = 1 << bit
    return index + size * (1 - 2 * (lax.div(index, size) % 2))


def first_update(grad):
    return grad / (jnp.abs(grad) + adam_epsilon)


def second_update(earlier, grad):
    first = (beta_one * (1.0 - beta_one)) * earlier + (1.0 - beta_one) * grad
    second = (beta_two * (1.0 - beta_two)) * earlier * earlier + (1.0 - beta_two) * grad * grad
    first_hat = first * (1.0 / (1.0 - beta_one**2))
    second_hat = second * (1.0 / (1.0 - beta_two**2))
    return first_hat / (jnp.sqrt(second_hat) + adam_epsilon)


def kernel(
    n_i, n_s, low_ref, gain_ref, rows_ref, stream_ref, goals_ref, total_ref, gain_total_ref,
    rows, anchor, later, grads, res, slope_low, stream, goals, from_left, from_right,
    stats, line, gains, gain_moves,
    local_sem, z_send, z_recv, a_send, a_recv, s_send, s_recv, g_send, g_recv, r_send, r_recv,
):
    i = lax.axis_index("island")
    s = lax.axis_index("shard")
    steps, _, block, width = rows.shape
    piece, cols = low_ref.shape
    tokens = n_s * block
    tiles = tokens // LANES
    scale = width ** (-0.5)
    depth = min(512, piece)
    tall = min(256, piece)

    barrier = pltpu.get_barrier_semaphore()
    for d in range(1, n_i):
        pl.semaphore_signal(barrier, inc=1, device_id=(lax.rem(i + d, n_i), s), device_id_type=MESH)
    for d in range(1, n_s):
        pl.semaphore_signal(barrier, inc=1, device_id=(i, lax.rem(s + d, n_s)), device_id_type=MESH)

    locals_ = [pltpu.make_async_copy(low_ref, anchor.at[i], local_sem.at[0])]
    for st in range(steps):
        locals_.append(pltpu.make_async_copy(rows_ref.at[0, st], rows.at[st, s], local_sem.at[1 + st]))
    locals_.append(pltpu.make_async_copy(stream_ref.at[0], stream, local_sem.at[1 + steps]))
    locals_.append(pltpu.make_async_copy(goals_ref.at[0], goals, local_sem.at[2 + steps]))
    for copy in locals_:
        copy.start()
    pl.semaphore_wait(barrier, n_i - 1 + n_s - 1)

    def remote(src, dst, send, recv, to):
        return pltpu.make_async_remote_copy(
            src_ref=src, dst_ref=dst, send_sem=send, recv_sem=recv, device_id=to, device_id_type=MESH
        )

    right, left = (lax.rem(i + 1, n_i), s), (lax.rem(i + n_i - 1, n_i), s)

    def z_copy(way, t, at):
        return remote(
            anchor.at[at], anchor.at[at], z_send.at[way, t], z_recv.at[way, t], right if way == 0 else left
        )

    def z_start(t):
        @pl.when((i < n_i - 1) & (i - t >= 0))
        def _():
            z_copy(0, t, i - t).start()

        @pl.when((i > 0) & (i + t <= n_i - 1))
        def _():
            z_copy(1, t, i + t).start()

    def z_wait(t):
        @pl.when(i - 1 - t >= 0)
        def _():
            z_copy(0, t, i - 1 - t).wait_recv()

        @pl.when(i + 1 + t <= n_i - 1)
        def _():
            z_copy(1, t, i + 1 + t).wait_recv()

    n_bits = n_s.bit_length() - 1
    orders = [list(range(1, n_bits)) + [0], list(range(n_bits - 1, 0, -1)) + [0]]

    def a_blocks(st, phase):
        order = orders[st % 2]
        found = []
        for m in range(1 << phase):
            at = s
            for q in range(phase):
                if (m >> q) & 1:
                    at = flip(at, order[q])
            found.append(at)
        return found

    def a_copy(st, phase, m, at):
        slot = (1 << phase) - 1 + m
        return remote(
            rows.at[st, at], rows.at[st, at], a_send.at[st, slot], a_recv.at[st, slot],
            (i, flip(s, orders[st % 2][phase])),
        )

    def a_start(phase):
        for st in range(steps):
            for m, at in enumerate(a_blocks(st, phase)):
                a_copy(st, phase, m, at).start()

    def a_wait(phase):
        for st in range(steps):
            for m, at in enumerate(a_blocks(st, phase)):
                a_copy(st, phase, m, flip(at, orders[st % 2][phase])).wait_recv()

    def to_islands(buffer, which):
        return [
            remote(
                buffer.at[0], buffer.at[d], g_send.at[which, d], g_recv.at[which, d],
                (lax.rem(i + d, n_i), s),
            )
            for d in range(1, n_i)
        ]

    locals_[0].wait()
    z_start(0)
    for copy in locals_[1 : 1 + steps]:
        copy.wait()
    a_start(0)
    gains[0] = gain_ref[...]
    gain_in = to_islands(gains, 0)
    for copy in gain_in:
        copy.start()
    res[...] = jnp.zeros_like(res)
    for copy in locals_[1 + steps :]:
        copy.wait()

    def project(st, weights, at):
        def body(k, _):
            start = pl.multiple_of(k * depth, depth)
            wide = pl.multiple_of(at * piece + k * depth, depth)
            part = rows[st, :, :, pl.ds(wide, depth)].reshape(tokens, depth)
            res[...] += jnp.dot(part, weights[at, pl.ds(start, depth), :], preferred_element_type=jnp.float32)
            return 0

        lax.fori_loop(0, piece // depth, body, 0)

    def project_arrived(t):
        @pl.when(i - 1 - t >= 0)
        def _():
            project(0, anchor, i - 1 - t)

        @pl.when(i + 1 + t <= n_i - 1)
        def _():
            project(0, anchor, i + 1 + t)

    events = [(2.0 * t + 2.6, "z", t) for t in range(n_i - 1)]
    events += [(2.0 * ((2 << p) - 1), "a", p) for p in range(n_bits - 1)]
    last = events[-1][0] if n_bits > 1 else 0.0
    events.append((last + 0.1, "a", n_bits - 1))
    gathered, ready = False, []
    for _, kind, at in sorted(events):
        if kind == "a":
            a_wait(at)
            if at + 1 < n_bits:
                a_start(at + 1)
            else:
                gathered = True
                project(0, anchor, i)
                for t in ready:
                    project_arrived(t)
        else:
            z_wait(at)
            if at + 1 < n_i - 1:
                z_start(at + 1)
            if gathered:
                project_arrived(at)
            else:
                ready.append(at)

    for copy in gain_in:
        copy.wait()
    gain_anchor = gains[0]
    for d in range(1, n_i):
        gain_anchor = gain_anchor + gains[d]
    gain = gain_anchor

    def fold(value):
        total = value[:, :LANES]
        for c in range(1, cols // LANES):
            total = total + value[:, c * LANES : (c + 1) * LANES]
        return jnp.sum(total.T, axis=0, keepdims=True)

    def spread(value):
        square = jnp.broadcast_to(value, (LANES, LANES)).T
        return jnp.concatenate([square] * (cols // LANES), axis=1)

    def row_stats(st, gain):
        def body(q, _):
            at = pl.ds(pl.multiple_of(q * LANES, LANES), LANES)
            r = stream[st, at, :].astype(jnp.float32) + res[at, :] * scale
            res[at, :] = r
            weighted = r * gain
            stats[st, 0, 0:1, at] = fold(r * r)
            stats[st, 0, 1:2, at] = fold(weighted * weighted)
            stats[st, 0, 2:3, at] = fold(weighted * goals[st, at, :].astype(jnp.float32))
            stats[st, 0, 3:4, at] = jnp.zeros((1, LANES), jnp.float32)
            return 0

        lax.fori_loop(0, tiles, body, 0)
        copies = [
            remote(
                stats.at[st, 0], stats.at[st, d], s_send.at[st, d], s_recv.at[st, d],
                (i, lax.rem(s + d, n_s)),
            )
            for d in range(1, n_s)
        ]
        for copy in copies:
            copy.start()
        for copy in copies:
            copy.wait()
        total = stats[st, 0]
        for d in range(1, n_s):
            total = total + stats[st, d]
        inverse = lax.rsqrt(total[0:1] * (1.0 / width) + norm_epsilon)
        slope = inverse * total[1:2] - total[2:3]
        line[0:1, :] = inverse
        line[1:2, :] = inverse * inverse * inverse * slope * (1.0 / width)

    def row_grads(st, gain):
        def body(q, total):
            at = pl.ds(pl.multiple_of(q * LANES, LANES), LANES)
            inverse, pull = spread(line[0:1, at]), spread(line[1:2, at])
            r = res[at, :]
            unit = r * inverse
            loss = unit * gain - goals[st, at, :].astype(jnp.float32)
            loss = loss.astype(jnp.bfloat16).astype(jnp.float32)
            slope_low[at, :] = (inverse * (loss * gain) - r * pull).astype(jnp.bfloat16)
            return total + jnp.sum(loss * unit, axis=0, keepdims=True)

        return lax.fori_loop(0, tiles, body, jnp.zeros((1, cols), jnp.float32))

    def weight_grad(st, wide):
        part = rows[st, :, :, pl.ds(pl.multiple_of(wide, tall), tall)].reshape(tokens, tall)
        return (
            lax.dot_general(
                part, slope_low[...], (((0,), (0,)), ((), ())), preferred_element_type=jnp.float32
            )
            * scale
        )

    row_stats(0, gain)
    gain_first = row_grads(0, gain)
    per_piece = piece // tall

    def step_one(q, _):
        o, j = q // per_piece, q % per_piece
        at = pl.ds(pl.multiple_of(j * tall, tall), tall)
        grad = weight_grad(0, q * tall)
        grads[o, at, :] = grad
        param = keep * anchor[o, at, :].astype(jnp.float32) - inner_rate * first_update(grad)
        later[o, at, :] = param.astype(jnp.bfloat16)
        return 0

    lax.fori_loop(0, n_i * per_piece, step_one, 0)
    gain_step = first_update(gain_first)
    gain = gain_anchor - inner_rate * gain_step

    res[...] = jnp.zeros_like(res)

    def project_later(at, _):
        project(1, later, at)
        return 0

    lax.fori_loop(0, n_i, project_later, 0)
    row_stats(1, gain)
    gain_second = row_grads(1, gain)
    gain_moves[0] = inner_rate * (gain_step + second_update(gain_first, gain_second))
    gain_out = to_islands(gain_moves, 1)
    for copy in gain_out:
        copy.start()

    def to_right(k):
        at = n_i - 1 - k
        return remote(later.at[at], from_left.at[k], r_send.at[0, k], r_recv.at[0, k], right)

    def to_left(k):
        return remote(later.at[k], from_right.at[k], r_send.at[1, k], r_recv.at[1, k], left)

    order = []
    for k in range((n_i + 1) // 2):
        order += [n_i - 1 - k] + ([k] if k != n_i - 1 - k else [])
    for o in order:

        def step_two(j, _, o=o):
            at = pl.ds(pl.multiple_of(j * tall, tall), tall)
            grad = weight_grad(1, o * piece + j * tall)
            earlier = grads[o, at, :]
            moved = (1.0 - keep * keep) * anchor[o, at, :].astype(jnp.float32) + inner_rate * (
                keep * first_update(earlier) + second_update(earlier, grad)
            )
            grads[o, at, :] = moved
            later[o, at, :] = moved.astype(jnp.bfloat16)
            return 0

        lax.fori_loop(0, per_piece, step_two, 0)
        if o > 0:

            @pl.when(i == 0)
            def _():
                to_right(n_i - 1 - o).start()

        if o < n_i - 1:

            @pl.when(i == n_i - 1)
            def _():
                to_left(o).start()

    def add(o, arrived, k):
        def body(j, _):
            at = pl.ds(pl.multiple_of(j * tall, tall), tall)
            later[o, at, :] = (grads[o, at, :] + arrived[k, at, :].astype(jnp.float32)).astype(jnp.bfloat16)
            return 0

        lax.fori_loop(0, per_piece, body, 0)

    for t in range(n_i - 1):
        k_right = t - i
        k_left = t - (n_i - 1 - i)

        @pl.when((i > 0) & (k_right >= 0) & (k_right < n_i - 1 - i))
        def _():
            to_right(k_right).wait_recv()
            add(n_i - 1 - k_right, from_left, k_right)
            to_right(k_right).start()

        @pl.when((i < n_i - 1) & (k_left >= 0) & (k_left < i))
        def _():
            to_left(k_left).wait_recv()
            add(k_left, from_right, k_left)
            to_left(k_left).start()

    for copy in gain_out:
        copy.wait()
    gain_total = gain_moves[0]
    for d in range(1, n_i):
        gain_total = gain_total + gain_moves[d]
    gain_total_ref[...] = gain_total

    total_ref[...] = grads[i]

    @pl.when(i > 0)
    def _():
        k = n_i - 1 - i
        to_right(k).wait_recv()
        total_ref[...] += from_left[k].astype(jnp.float32)

    @pl.when(i < n_i - 1)
    def _():
        to_left(i).wait_recv()
        total_ref[...] += from_right[i].astype(jnp.float32)

    for k in range(n_i - 1):

        @pl.when(k < n_i - 1 - i)
        def _(k=k):
            to_right(k).wait_send()

        @pl.when(k < i)
        def _(k=k):
            to_left(k).wait_send()

        @pl.when((i < n_i - 1) & (i - k >= 0))
        def _(k=k):
            z_copy(0, k, i - k).wait_send()

        @pl.when((i > 0) & (i + k <= n_i - 1))
        def _(k=k):
            z_copy(1, k, i + k).wait_send()

    for phase in range(n_bits):
        for st in range(steps):
            for m, at in enumerate(a_blocks(st, phase)):
                a_copy(st, phase, m, at).wait_send()


def per_device(weight_master, gain_master, weight_moment, gain_moment, attended, stream, targets):
    n_i, n_s = lax.axis_size("island"), lax.axis_size("shard")
    _, steps, block, width = attended.shape
    _, _, tokens, cols = stream.shape
    piece = weight_master.shape[0]
    own = gain_master.shape[0]
    offset = lax.axis_index("island") * own
    low = weight_master.astype(jnp.bfloat16)
    gain_low = gain_master.astype(jnp.bfloat16).astype(jnp.float32)
    gain_row = lax.dynamic_update_slice(jnp.zeros((1, cols), jnp.float32), gain_low[None], (0, offset))
    any_space = pl.BlockSpec(memory_space=pl.ANY)
    vmem = pl.BlockSpec(memory_space=pltpu.VMEM)
    f32, bf16 = jnp.float32, jnp.bfloat16
    dma = pltpu.SemaphoreType.DMA
    weight_summed, gain_summed = pl.pallas_call(
        functools.partial(kernel, n_i, n_s),
        out_shape=(
            jax.ShapeDtypeStruct((piece, cols), f32),
            jax.ShapeDtypeStruct((1, cols), f32),
        ),
        in_specs=[any_space, vmem, any_space, any_space, any_space],
        out_specs=(vmem, vmem),
        scratch_shapes=[
            pltpu.VMEM((steps, n_s, block, width), bf16),
            pltpu.VMEM((n_i, piece, cols), bf16),
            pltpu.VMEM((n_i, piece, cols), bf16),
            pltpu.VMEM((n_i, piece, cols), f32),
            pltpu.VMEM((tokens, cols), f32),
            pltpu.VMEM((tokens, cols), bf16),
            pltpu.VMEM((steps, tokens, cols), bf16),
            pltpu.VMEM((steps, tokens, cols), bf16),
            pltpu.VMEM((n_i - 1, piece, cols), bf16),
            pltpu.VMEM((n_i - 1, piece, cols), bf16),
            pltpu.VMEM((steps, n_s, 4, tokens), f32),
            pltpu.VMEM((2, tokens), f32),
            pltpu.VMEM((n_i, 1, cols), f32),
            pltpu.VMEM((n_i, 1, cols), f32),
            dma((3 + steps,)),
            dma((2, n_i - 1)),
            dma((2, n_i - 1)),
            dma((steps, n_s - 1)),
            dma((steps, n_s - 1)),
            dma((steps, n_s)),
            dma((steps, n_s)),
            dma((2, n_i)),
            dma((2, n_i)),
            dma((2, n_i - 1)),
            dma((2, n_i - 1)),
        ],
        compiler_params=pltpu.CompilerParams(
            collective_id=0, has_side_effects=True, vmem_limit_bytes=67043328
        ),
    )(low, gain_row, attended, stream, targets)
    weight_pseudo = weight_summed / n_i
    gain_pseudo = lax.dynamic_slice(gain_summed, (0, offset), (1, own))[0] / n_i
    weight_velocity = outer_momentum * weight_moment + weight_pseudo
    gain_velocity = outer_momentum * gain_moment + gain_pseudo
    weight_updated = weight_master - outer_rate * (weight_pseudo + outer_momentum * weight_velocity)
    gain_updated = gain_master - outer_rate * (gain_pseudo + outer_momentum * gain_velocity)
    return (weight_updated, gain_updated, weight_velocity, gain_velocity)


def solution(mesh):
    placed = (
        P("island", "shard"),
        P(("shard", "island")),
        P("island", "shard"),
        P(("shard", "island")),
        P("island", None, "shard", None),
        P("island", None, None, "shard"),
        P("island", None, None, "shard"),
    )
    return jax.shard_map(
        per_device,
        mesh=mesh,
        in_specs=placed,
        out_specs=(
            P("island", "shard"),
            P(("shard", "island")),
            P("island", "shard"),
            P(("shard", "island")),
        ),
        check_vma=False,
    )
```

```python
import functools

import jax
import jax.numpy as jnp
from jax import lax
from jax.experimental import pallas as pl
from jax.experimental.pallas import tpu as pltpu
from jax.sharding import PartitionSpec as P

norm_epsilon = 1e-05
inner_rate = 0.05
beta_one = 0.9
beta_two = 0.95
adam_epsilon = 0.3
decay_rate = 0.1
outer_rate = 0.7
outer_momentum = 0.9

MESH = pl.DeviceIdType.MESH
LANES = 128
keep = 1.0 - inner_rate * decay_rate


def flip(index, bit):
    size = 1 << bit
    return index + size * (1 - 2 * (lax.div(index, size) % 2))


def first_update(grad):
    return grad / (jnp.abs(grad) + adam_epsilon)


def second_update(earlier, grad):
    first = (beta_one * (1.0 - beta_one)) * earlier + (1.0 - beta_one) * grad
    second = (beta_two * (1.0 - beta_two)) * earlier * earlier + (1.0 - beta_two) * grad * grad
    first_hat = first * (1.0 / (1.0 - beta_one**2))
    second_hat = second * (1.0 / (1.0 - beta_two**2))
    return first_hat / (jnp.sqrt(second_hat) + adam_epsilon)


def kernel(
    n_i, n_s, low_ref, gain_ref, rows_ref, stream_ref, goals_ref, total_ref, gain_total_ref,
    rows, anchor, later, grads, res, slope_low, stream, goals, from_left, from_right,
    stats, line, gains, gain_moves,
    local_sem, z_send, z_recv, a_send, a_recv, s_send, s_recv, g_send, g_recv, r_send, r_recv,
):
    i = lax.axis_index("island")
    s = lax.axis_index("shard")
    steps, _, block, width = rows.shape
    piece, cols = low_ref.shape
    tokens = n_s * block
    tiles = tokens // LANES
    scale = width ** (-0.5)
    depth = min(512, piece)
    tall = min(256, piece)

    barrier = pltpu.get_barrier_semaphore()
    for d in range(1, n_i):
        pl.semaphore_signal(barrier, inc=1, device_id=(lax.rem(i + d, n_i), s), device_id_type=MESH)
    for d in range(1, n_s):
        pl.semaphore_signal(barrier, inc=1, device_id=(i, lax.rem(s + d, n_s)), device_id_type=MESH)

    locals_ = [pltpu.make_async_copy(low_ref, anchor.at[i], local_sem.at[0])]
    for st in range(steps):
        locals_.append(pltpu.make_async_copy(rows_ref.at[0, st], rows.at[st, s], local_sem.at[1 + st]))
    locals_.append(pltpu.make_async_copy(stream_ref.at[0], stream, local_sem.at[1 + steps]))
    locals_.append(pltpu.make_async_copy(goals_ref.at[0], goals, local_sem.at[2 + steps]))
    for copy in locals_:
        copy.start()
    pl.semaphore_wait(barrier, n_i - 1 + n_s - 1)

    def remote(src, dst, send, recv, to):
        return pltpu.make_async_remote_copy(
            src_ref=src, dst_ref=dst, send_sem=send, recv_sem=recv, device_id=to, device_id_type=MESH
        )

    right, left = (lax.rem(i + 1, n_i), s), (lax.rem(i + n_i - 1, n_i), s)

    def z_copy(way, t, at):
        return remote(
            anchor.at[at], anchor.at[at], z_send.at[way, t], z_recv.at[way, t], right if way == 0 else left
        )

    def z_start(t):
        @pl.when((i < n_i - 1) & (i - t >= 0))
        def _():
            z_copy(0, t, i - t).start()

        @pl.when((i > 0) & (i + t <= n_i - 1))
        def _():
            z_copy(1, t, i + t).start()

    def z_wait(t):
        @pl.when(i - 1 - t >= 0)
        def _():
            z_copy(0, t, i - 1 - t).wait_recv()

        @pl.when(i + 1 + t <= n_i - 1)
        def _():
            z_copy(1, t, i + 1 + t).wait_recv()

    n_bits = n_s.bit_length() - 1
    orders = [list(range(1, n_bits)) + [0], list(range(n_bits - 1, 0, -1)) + [0]]

    def a_blocks(st, phase):
        order = orders[st % 2]
        found = []
        for m in range(1 << phase):
            at = s
            for q in range(phase):
                if (m >> q) & 1:
                    at = flip(at, order[q])
            found.append(at)
        return found

    def a_copy(st, phase, m, at):
        slot = (1 << phase) - 1 + m
        return remote(
            rows.at[st, at], rows.at[st, at], a_send.at[st, slot], a_recv.at[st, slot],
            (i, flip(s, orders[st % 2][phase])),
        )

    def a_start(phase):
        for st in range(steps):
            for m, at in enumerate(a_blocks(st, phase)):
                a_copy(st, phase, m, at).start()

    def a_wait(phase):
        for st in range(steps):
            for m, at in enumerate(a_blocks(st, phase)):
                a_copy(st, phase, m, flip(at, orders[st % 2][phase])).wait_recv()

    def to_islands(buffer, which):
        return [
            remote(
                buffer.at[0], buffer.at[d], g_send.at[which, d], g_recv.at[which, d],
                (lax.rem(i + d, n_i), s),
            )
            for d in range(1, n_i)
        ]

    locals_[0].wait()
    z_start(0)
    for copy in locals_[1 : 1 + steps]:
        copy.wait()
    a_start(0)
    gains[0] = gain_ref[...]
    gain_in = to_islands(gains, 0)
    for copy in gain_in:
        copy.start()
    res[...] = jnp.zeros_like(res)
    for copy in locals_[1 + steps :]:
        copy.wait()

    def project(st, weights, at):
        def body(k, _):
            start = pl.multiple_of(k * depth, depth)
            wide = pl.multiple_of(at * piece + k * depth, depth)
            part = rows[st, :, :, pl.ds(wide, depth)].reshape(tokens, depth)
            res[...] += jnp.dot(part, weights[at, pl.ds(start, depth), :], preferred_element_type=jnp.float32)
            return 0

        lax.fori_loop(0, piece // depth, body, 0)

    def project_arrived(t):
        @pl.when(i - 1 - t >= 0)
        def _():
            project(0, anchor, i - 1 - t)

        @pl.when(i + 1 + t <= n_i - 1)
        def _():
            project(0, anchor, i + 1 + t)

    events = [(2.0 * t + 2.6, "z", t) for t in range(n_i - 1)]
    events += [(2.0 * ((2 << p) - 1), "a", p) for p in range(n_bits - 1)]
    last = events[-1][0] if n_bits > 1 else 0.0
    events.append((last + 0.1, "a", n_bits - 1))
    gathered, ready = False, []
    for _, kind, at in sorted(events):
        if kind == "a":
            a_wait(at)
            if at + 1 < n_bits:
                a_start(at + 1)
            else:
                gathered = True
                project(0, anchor, i)
                for t in ready:
                    project_arrived(t)
        else:
            z_wait(at)
            if at + 1 < n_i - 1:
                z_start(at + 1)
            if gathered:
                project_arrived(at)
            else:
                ready.append(at)

    for copy in gain_in:
        copy.wait()
    gain_anchor = gains[0]
    for d in range(1, n_i):
        gain_anchor = gain_anchor + gains[d]
    gain = gain_anchor

    def fold(value):
        total = value[:, :LANES]
        for c in range(1, cols // LANES):
            total = total + value[:, c * LANES : (c + 1) * LANES]
        return jnp.sum(total.T, axis=0, keepdims=True)

    def spread(value):
        square = jnp.broadcast_to(value, (LANES, LANES)).T
        return jnp.concatenate([square] * (cols // LANES), axis=1)

    def row_stats(st, gain):
        def body(q, _):
            at = pl.ds(pl.multiple_of(q * LANES, LANES), LANES)
            r = stream[st, at, :].astype(jnp.float32) + res[at, :] * scale
            res[at, :] = r
            weighted = r * gain
            stats[st, 0, 0:1, at] = fold(r * r)
            stats[st, 0, 1:2, at] = fold(weighted * weighted)
            stats[st, 0, 2:3, at] = fold(weighted * goals[st, at, :].astype(jnp.float32))
            stats[st, 0, 3:4, at] = jnp.zeros((1, LANES), jnp.float32)
            return 0

        lax.fori_loop(0, tiles, body, 0)
        copies = [
            remote(
                stats.at[st, 0], stats.at[st, d], s_send.at[st, d], s_recv.at[st, d],
                (i, lax.rem(s + d, n_s)),
            )
            for d in range(1, n_s)
        ]
        for copy in copies:
            copy.start()
        for copy in copies:
            copy.wait()
        total = stats[st, 0]
        for d in range(1, n_s):
            total = total + stats[st, d]
        inverse = lax.rsqrt(total[0:1] * (1.0 / width) + norm_epsilon)
        slope = inverse * total[1:2] - total[2:3]
        line[0:1, :] = inverse
        line[1:2, :] = inverse * inverse * inverse * slope * (1.0 / width)

    def row_grads(st, gain):
        def body(q, total):
            at = pl.ds(pl.multiple_of(q * LANES, LANES), LANES)
            inverse, pull = spread(line[0:1, at]), spread(line[1:2, at])
            r = res[at, :]
            unit = r * inverse
            loss = unit * gain - goals[st, at, :].astype(jnp.float32)
            loss = loss.astype(jnp.bfloat16).astype(jnp.float32)
            slope_low[at, :] = (inverse * (loss * gain) - r * pull).astype(jnp.bfloat16)
            return total + jnp.sum(loss * unit, axis=0, keepdims=True)

        return lax.fori_loop(0, tiles, body, jnp.zeros((1, cols), jnp.float32))

    def weight_grad(st, wide):
        part = rows[st, :, :, pl.ds(pl.multiple_of(wide, tall), tall)].reshape(tokens, tall)
        return (
            lax.dot_general(
                part, slope_low[...], (((0,), (0,)), ((), ())), preferred_element_type=jnp.float32
            )
            * scale
        )

    row_stats(0, gain)
    gain_first = row_grads(0, gain)
    per_piece = piece // tall

    def step_one(q, _):
        o, j = q // per_piece, q % per_piece
        at = pl.ds(pl.multiple_of(j * tall, tall), tall)
        grad = weight_grad(0, q * tall)
        grads[o, at, :] = grad
        param = keep * anchor[o, at, :].astype(jnp.float32) - inner_rate * first_update(grad)
        later[o, at, :] = param.astype(jnp.bfloat16)
        return 0

    lax.fori_loop(0, n_i * per_piece, step_one, 0)
    gain_step = first_update(gain_first)
    gain = gain_anchor - inner_rate * gain_step

    res[...] = jnp.zeros_like(res)

    def project_later(at, _):
        project(1, later, at)
        return 0

    lax.fori_loop(0, n_i, project_later, 0)
    row_stats(1, gain)
    gain_second = row_grads(1, gain)
    gain_moves[0] = inner_rate * (gain_step + second_update(gain_first, gain_second))
    gain_out = to_islands(gain_moves, 1)
    for copy in gain_out:
        copy.start()

    def to_right(k):
        at = n_i - 1 - k
        return remote(later.at[at], from_left.at[k], r_send.at[0, k], r_recv.at[0, k], right)

    def to_left(k):
        return remote(later.at[k], from_right.at[k], r_send.at[1, k], r_recv.at[1, k], left)

    early = 1 - lax.div(2 * i, n_i)

    def owner_piece(q, _):
        o = q + early * (n_i - 1 - 2 * q)

        def step_two(j, _):
            at = pl.ds(pl.multiple_of(j * tall, tall), tall)
            grad = weight_grad(1, o * piece + j * tall)
            earlier = grads[o, at, :]
            moved = (1.0 - keep * keep) * anchor[o, at, :].astype(jnp.float32) + inner_rate * (
                keep * first_update(earlier) + second_update(earlier, grad)
            )
            grads[o, at, :] = moved
            later[o, at, :] = moved.astype(jnp.bfloat16)
            return 0

        lax.fori_loop(0, per_piece, step_two, 0)

        @pl.when((i == 0) & (o > 0))
        def _():
            to_right(n_i - 1 - o).start()

        @pl.when((i == n_i - 1) & (o < n_i - 1))
        def _():
            to_left(o).start()

        return 0

    lax.fori_loop(0, n_i, owner_piece, 0)

    def add(o, arrived, k):
        def body(j, _):
            at = pl.ds(pl.multiple_of(j * tall, tall), tall)
            later[o, at, :] = (grads[o, at, :] + arrived[k, at, :].astype(jnp.float32)).astype(jnp.bfloat16)
            return 0

        lax.fori_loop(0, per_piece, body, 0)

    for t in range(n_i - 1):
        k_right = t - i
        k_left = t - (n_i - 1 - i)

        @pl.when((i > 0) & (k_right >= 0) & (k_right < n_i - 1 - i))
        def _():
            to_right(k_right).wait_recv()
            add(n_i - 1 - k_right, from_left, k_right)
            to_right(k_right).start()

        @pl.when((i < n_i - 1) & (k_left >= 0) & (k_left < i))
        def _():
            to_left(k_left).wait_recv()
            add(k_left, from_right, k_left)
            to_left(k_left).start()

    for copy in gain_out:
        copy.wait()
    gain_total = gain_moves[0]
    for d in range(1, n_i):
        gain_total = gain_total + gain_moves[d]
    gain_total_ref[...] = gain_total

    total_ref[...] = grads[i]

    @pl.when(i > 0)
    def _():
        k = n_i - 1 - i
        to_right(k).wait_recv()
        total_ref[...] += from_left[k].astype(jnp.float32)

    @pl.when(i < n_i - 1)
    def _():
        to_left(i).wait_recv()
        total_ref[...] += from_right[i].astype(jnp.float32)

    for k in range(n_i - 1):

        @pl.when(k < n_i - 1 - i)
        def _(k=k):
            to_right(k).wait_send()

        @pl.when(k < i)
        def _(k=k):
            to_left(k).wait_send()

        @pl.when((i < n_i - 1) & (i - k >= 0))
        def _(k=k):
            z_copy(0, k, i - k).wait_send()

        @pl.when((i > 0) & (i + k <= n_i - 1))
        def _(k=k):
            z_copy(1, k, i + k).wait_send()

    for phase in range(n_bits):
        for st in range(steps):
            for m, at in enumerate(a_blocks(st, phase)):
                a_copy(st, phase, m, at).wait_send()


def per_device(weight_master, gain_master, weight_moment, gain_moment, attended, stream, targets):
    n_i, n_s = lax.axis_size("island"), lax.axis_size("shard")
    _, steps, block, width = attended.shape
    _, _, tokens, cols = stream.shape
    piece = weight_master.shape[0]
    own = gain_master.shape[0]
    offset = lax.axis_index("island") * own
    low = weight_master.astype(jnp.bfloat16)
    gain_low = gain_master.astype(jnp.bfloat16).astype(jnp.float32)
    gain_row = lax.dynamic_update_slice(jnp.zeros((1, cols), jnp.float32), gain_low[None], (0, offset))
    any_space = pl.BlockSpec(memory_space=pl.ANY)
    vmem = pl.BlockSpec(memory_space=pltpu.VMEM)
    f32, bf16 = jnp.float32, jnp.bfloat16
    dma = pltpu.SemaphoreType.DMA
    weight_summed, gain_summed = pl.pallas_call(
        functools.partial(kernel, n_i, n_s),
        out_shape=(
            jax.ShapeDtypeStruct((piece, cols), f32),
            jax.ShapeDtypeStruct((1, cols), f32),
        ),
        in_specs=[any_space, vmem, any_space, any_space, any_space],
        out_specs=(vmem, vmem),
        scratch_shapes=[
            pltpu.VMEM((steps, n_s, block, width), bf16),
            pltpu.VMEM((n_i, piece, cols), bf16),
            pltpu.VMEM((n_i, piece, cols), bf16),
            pltpu.VMEM((n_i, piece, cols), f32),
            pltpu.VMEM((tokens, cols), f32),
            pltpu.VMEM((tokens, cols), bf16),
            pltpu.VMEM((steps, tokens, cols), bf16),
            pltpu.VMEM((steps, tokens, cols), bf16),
            pltpu.VMEM((n_i - 1, piece, cols), bf16),
            pltpu.VMEM((n_i - 1, piece, cols), bf16),
            pltpu.VMEM((steps, n_s, 4, tokens), f32),
            pltpu.VMEM((2, tokens), f32),
            pltpu.VMEM((n_i, 1, cols), f32),
            pltpu.VMEM((n_i, 1, cols), f32),
            dma((3 + steps,)),
            dma((2, n_i - 1)),
            dma((2, n_i - 1)),
            dma((steps, n_s - 1)),
            dma((steps, n_s - 1)),
            dma((steps, n_s)),
            dma((steps, n_s)),
            dma((2, n_i)),
            dma((2, n_i)),
            dma((2, n_i - 1)),
            dma((2, n_i - 1)),
        ],
        compiler_params=pltpu.CompilerParams(
            collective_id=0, has_side_effects=True, vmem_limit_bytes=67043328
        ),
    )(low, gain_row, attended, stream, targets)
    weight_pseudo = weight_summed / n_i
    gain_pseudo = lax.dynamic_slice(gain_summed, (0, offset), (1, own))[0] / n_i
    weight_velocity = outer_momentum * weight_moment + weight_pseudo
    gain_velocity = outer_momentum * gain_moment + gain_pseudo
    weight_updated = weight_master - outer_rate * (weight_pseudo + outer_momentum * weight_velocity)
    gain_updated = gain_master - outer_rate * (gain_pseudo + outer_momentum * gain_velocity)
    return (weight_updated, gain_updated, weight_velocity, gain_velocity)


def solution(mesh):
    placed = (
        P("island", "shard"),
        P(("shard", "island")),
        P("island", "shard"),
        P(("shard", "island")),
        P("island", None, "shard", None),
        P("island", None, None, "shard"),
        P("island", None, None, "shard"),
    )
    return jax.shard_map(
        per_device,
        mesh=mesh,
        in_specs=placed,
        out_specs=(
            P("island", "shard"),
            P(("shard", "island")),
            P("island", "shard"),
            P(("shard", "island")),
        ),
        check_vma=False,
    )
```
